32 devices in a mesh: band: 8 (over z, x), patch: 4 (over y, core).
Axes of the slice: x: 2, y: 2, z: 4, core: 2. Of those that a mesh axis runs over, the one named last changes fastest.
Arguments:
- latents: bfloat16 [8, 10240, 512], P('band', 'patch'), may hold values from -6 to 6
- owners: int32 [16], replicated, may hold values from 0 to 3, as said below
- block_rows: int32 [16, 128], replicated, may hold values from 0 to 2559
- interp_weights: bfloat16 [16, 1024, 128], P('band', 'patch'), may hold values from -0.5 to 0.5
- w_first: bfloat16 [8, 512, 512], P('band'), may hold values from -0.25 to 0.25
- b_first: float32 [8, 512], P('band'), may hold values from -3 to 3
- w_second: bfloat16 [8, 512, 512], P('band'), may hold values from -0.25 to 0.25
- b_second: float32 [8, 512], P('band'), may hold values from -4 to 4
- gain: float32 [8, 512], P('band'), may hold values from 0.1 to 1.9
- w_out: bfloat16 [8, 12, 512], P('band'), may hold values from -0.25 to 0.25
- b_out: float32 [8, 12], P('band'), may hold values from -4 to 4
Outputs:
- grid_fields: float32 [8, 12, 16384], P('band', None, 'patch')
The draws below stay inside these ranges and needn't reach their ends.
Inputs may be any that keep to these rules, and one draw needn't show every extreme that they name: `owners`: no patch owns more than 8 tiles, and one patch owns exactly 8.
All inputs are finite; a program needn't handle non-finite values.
Results may differ from the reference program's by a relative error of at most 0.003.
Values may be sent and summed in bfloat16 or wider, within the bound.
A program may use at most 64 MiB of HBM per device.

```python
import jax
import jax.numpy as jnp
from jax import lax

D = 512
BLK = 128
TILES = 16
MESH_DEV = 2560
CH = 12
CAP = 8
CELLS_T = 1024
MESH = 10240
BANDS = 8
N_PATCH = 4


def draw_owners(key, part):
    key_heavy, key_order, key_offset = jax.random.split(jax.random.fold_in(key, 11), 3)
    heavy_owner = jax.random.randint(key_heavy, (), 0, N_PATCH)
    tile_order = jax.random.permutation(key_order, TILES)
    offset_draw = jax.random.randint(key_offset, (), 0, N_PATCH - 1)
    position = jnp.arange(TILES)
    others = (heavy_owner + 1 + (position - CAP + offset_draw) % (N_PATCH - 1)) % N_PATCH
    owner_by_position = jnp.where(position < CAP, heavy_owner, others).astype(jnp.int32)
    return jnp.zeros((TILES,), jnp.int32).at[tile_order].set(owner_by_position)


def place_ends(drawn, own_key, smallest, high):
    extent = drawn.shape
    spot = [jax.random.randint(jax.random.fold_in(own_key, axis), (), 0, extent[axis]) for axis in range(len(extent))]
    drawn = drawn.at[tuple(spot)].set(smallest)
    longest = extent.index(max(extent))
    spot[longest] = (spot[longest] + 1) % extent[longest]
    return drawn.at[tuple(spot)].set(high)


def steps_of(own_key, shape, pieces, low, top_value):
    loudness = 1.0
    for axis_at, shards_of in pieces:
        steps = jax.random.uniform(jax.random.fold_in(jax.random.fold_in(own_key, 6), axis_at), (shards_of,), jnp.float32, low / len(pieces), top_value / len(pieces))
        loudness = loudness * jnp.repeat(jnp.exp(steps), shape[axis_at] // shards_of).reshape((-1,) + (1,) * (len(shape) - 1 - axis_at))
    return loudness


def noise(own_key, extent, spread, limit, pieces=(), kind=jnp.bfloat16):
    array = spread * jax.random.normal(own_key, extent, jnp.float32)
    if pieces:
        array = array * steps_of(own_key, extent, pieces, -0.22, 0.18)
    return jnp.clip(array, -limit, limit).astype(kind)


def setup_inputs(seed: int = 0) -> dict:
    keys = jax.random.split(jax.random.key(seed), 12)
    latents = noise(keys[0], (BANDS, MESH, D), 1.0, 6.0, ((0, 8), (1, 4)))
    owners = draw_owners(jax.random.fold_in(keys[11], 71), 0)
    block_rows = place_ends(jax.random.randint(keys[2], (TILES, BLK), 0, MESH_DEV), jax.random.fold_in(keys[2], 1), 0, MESH_DEV - 1).astype(jnp.int32)
    interp_weights = noise(keys[3], (TILES, CELLS_T, BLK), BLK ** -0.5, 0.5, ((0, 8), (1, 4)))
    w_first = noise(keys[4], (BANDS, D, D), D ** -0.5, 0.25, ((0, 8),))
    b_first = noise(keys[5], (BANDS, D), 0.5, 3.0, ((0, 8),), jnp.float32)
    w_second = noise(keys[6], (BANDS, D, D), D ** -0.5, 0.25, ((0, 8),))
    b_second = noise(keys[7], (BANDS, D), 1.0, 4.0, ((0, 8),), jnp.float32)
    gain = jnp.clip(1.0 + 0.18 * jax.random.normal(keys[8], (BANDS, D), jnp.float32), 0.1, 1.9)
    w_out = noise(keys[9], (BANDS, CH, D), D ** -0.5, 0.25, ((0, 8),))
    b_out = noise(keys[10], (BANDS, CH), 1.0, 4.0, ((0, 8),), jnp.float32)
    return {"latents": latents, "owners": owners, "block_rows": block_rows, "interp_weights": interp_weights, "w_first": w_first, "b_first": b_first, "w_second": w_second, "b_second": b_second, "gain": gain, "w_out": w_out, "b_out": b_out}


def decode_rows(interp, w_first, b_first, w_second, b_second, gain, w_out, b_out):
    hidden = jax.nn.silu(jnp.dot(interp, w_first, preferred_element_type=jnp.float32) + b_first).astype(jnp.bfloat16)
    second = jnp.dot(hidden, w_second, preferred_element_type=jnp.float32) + b_second
    mean_value = lax.optimization_barrier(jnp.mean(second, axis=-1, keepdims=True))
    centred = second - mean_value
    variance = lax.optimization_barrier(jnp.mean(centred * centred, axis=-1, keepdims=True))
    normed = (centred * lax.rsqrt(variance + 1e-05) * gain).astype(jnp.bfloat16)
    result = lax.dot_general(w_out, normed, (((1,), (1,)), ((), ())), preferred_element_type=jnp.float32)
    return result + b_out[:, None]

def reference(latents, owners, block_rows, interp_weights, w_first, b_first, w_second, b_second, gain, w_out, b_out):
    mesh_dev = latents.shape[1] // N_PATCH

    def one_band(band_args):
        band_latents, first_w, first_b, second_w, second_b, band_gain, out_w, out_b = band_args

        def one_tile(tile_index):
            rows_global = owners[tile_index] * mesh_dev + block_rows[tile_index]
            block = jnp.take(band_latents, rows_global.astype(jnp.int32), axis=0)
            interp = jnp.dot(interp_weights[tile_index], block, preferred_element_type=jnp.float32).astype(jnp.bfloat16)
            return decode_rows(interp, first_w, first_b, second_w, second_b, band_gain, out_w, out_b)
        per_tile = lax.map(one_tile, jnp.arange(TILES, dtype=jnp.int32))
        return jnp.transpose(per_tile, (1, 0, 2)).reshape(per_tile.shape[1], -1)
    return lax.map(one_band, (latents, w_first, b_first, w_second, b_second, gain, w_out, b_out))
```

```python
import functools

import jax
import jax.numpy as jnp
from jax import lax
from jax.experimental import pallas as pl
from jax.experimental.pallas import tpu as pltpu
from jax.sharding import PartitionSpec as P

LEAD = 2


def kernel(
    nb, np_, tiles, blk, cl,
    owners, rows, w_b1, w_b2, w_gain, w_out, w_bo, latents, pieces, w_first, w_second,
    out,
    lat, w1, w2, perm, onehot, acc, sib, own, from_sib, from_chip, weights, block,
    lat_sem, wt_sem, piece_send, w_recv, w_send, sib_send, sib_recv, chip_send, chip_recv,
):
    b, p = lax.axis_index("band"), lax.axis_index("patch")
    n_chips = np_ // 2
    tb, tp = tiles // nb, tiles // np_
    g = tp // tb
    n_z = nb // 2
    q, c = p // 2, p % 2
    z, x = b // 2, b % 2
    units = g * tb * n_chips
    rows_u = 2 * cl
    mesh_dev, width = latents.shape
    depth = onehot.shape[1]
    mesh_type = pl.DeviceIdType.MESH

    def dev(band, patch):
        return {"band": band, "patch": patch}

    def remote(src, dst, send, recv, band, patch):
        return pltpu.make_async_remote_copy(
            src_ref=src, dst_ref=dst, send_sem=send, recv_sem=recv,
            device_id=dev(band, patch), device_id_type=mesh_type,
        )

    barrier = pltpu.get_barrier_semaphore()

    def greet(band, patch):
        pl.semaphore_signal(barrier, inc=1, device_id=dev(band, patch), device_id_type=mesh_type)

    for d in range(1, np_):
        greet(b, (p + d) % np_)
    greet(2 * z + 1 - x, p)

    @pl.when(z > 0)
    def _():
        greet(b - 2, p)

    @pl.when(z < n_z - 1)
    def _():
        greet(b + 2, p)

    lat_copies = [
        pltpu.make_async_copy(
            latents.at[pl.ds(k * depth, depth)], lat.at[pl.ds(k * depth, depth)], lat_sem.at[k]
        )
        for k in range(mesh_dev // depth)
    ]
    for copy in lat_copies:
        copy.start()
    w1_copy = pltpu.make_async_copy(w_first, w1, wt_sem.at[0])
    w2_copy = pltpu.make_async_copy(w_second, w2, wt_sem.at[1])
    w1_copy.start()
    w2_copy.start()

    offsets = list(range(1, n_chips)) + [0]
    order = []
    for d_list in (offsets[:-1], offsets[-1:]):
        for core in (1 - c, c):
            for d in d_list:
                for i in range(tp):
                    order.append((2 * ((q + d) % n_chips) + core) * tp + i)
    perm[...] = jnp.full(perm.shape, -1, jnp.int32)
    for k, t in enumerate(order):
        mine = (owners[t] == p).astype(jnp.int32)
        perm[k : k + 1, :] = rows[pl.ds(t, 1), :] * mine + (mine - 1)
    columns = perm[...].T

    pl.semaphore_wait(barrier, np_ + (z > 0).astype(jnp.int32) + (z < n_z - 1).astype(jnp.int32))

    home = b // g
    own_source = b % g
    piece_copies = [
        (
            pieces.at[i],
            weights.at[own_source * tb + i, pl.ds(pl.multiple_of(p * cl, cl), cl)],
            w_recv.at[own_source, i, q],
            piece_send.at[i],
        )
        for i in range(tb)
    ]

    @pl.when(p == home)
    def _():
        for src, dst, recv, _ in piece_copies:
            pltpu.make_async_copy(src, dst, recv).start()

    @pl.when(p != home)
    def _():
        for src, dst, recv, send in piece_copies:
            remote(src, dst, send, recv, b, home).start()

    def unit_of(n):
        jj, k = n % g, n // g
        i, dd = k // n_chips, k % n_chips
        j = (x + jj) % g
        qq = (q + dd) % n_chips
        return i, j, qq

    def chunk(n):
        i, j, qq = unit_of(n)
        return weights.at[j * tb + i, pl.ds(pl.multiple_of(qq * rows_u, rows_u), rows_u)]

    def forwards(n, act):
        i, j, qq = unit_of(n)
        source = p * g + j
        zs, xs = source // 2, source % 2
        part = chunk(n)
        recv = w_recv.at[j, i, qq]
        on_line = x == xs

        @pl.when(on_line & (z >= zs) & (z < n_z - 1))
        def _():
            act(remote(part, part, w_send.at[0, n], recv, b + 2, p))

        @pl.when(on_line & (z <= zs) & (z > 0))
        def _():
            act(remote(part, part, w_send.at[1, n], recv, b - 2, p))

        @pl.when(on_line)
        def _():
            act(remote(part, part, w_send.at[2, n], recv, 2 * z + 1 - x, p))

    def relay(n):
        i, j, qq = unit_of(n)
        part = chunk(n)
        pltpu.make_async_copy(part, part, w_recv.at[j, i, qq]).wait()
        forwards(n, lambda copy: copy.start())

    iota = lax.broadcasted_iota(jnp.int32, (blk, depth), 1)

    def gather(first, count, dst, first_time):
        for k in range(mesh_dev // depth):
            if first_time:
                lat_copies[k].wait()
            for r in range(count):
                hit = iota == (columns[:, first + r : first + r + 1] - k * depth)
                onehot[r * blk : (r + 1) * blk, :] = jnp.where(hit, 1.0, 0.0).astype(jnp.bfloat16)
            part = jnp.dot(
                onehot[: count * blk, :], lat[k * depth : (k + 1) * depth, :],
                preferred_element_type=jnp.float32,
            )
            if k:
                part = part + acc[: count * blk, :]
            if k < mesh_dev // depth - 1:
                acc[: count * blk, :] = part
            else:
                dst[...] = part.astype(jnp.bfloat16).reshape(dst.shape)

    def to_sibling(d, i):
        return remote(
            sib.at[d, i], from_sib.at[d, i], sib_send.at[d, i], sib_recv.at[d, i], b, 2 * q + 1 - c
        )

    def to_chip(d, i):
        return remote(
            own.at[d, i], from_chip.at[d - 1, i], chip_send.at[d - 1, i], chip_recv.at[d - 1, i],
            b, 2 * ((q + d) % n_chips) + c,
        )

    far = (n_chips - 1) * tp
    if n_chips > 1:
        gather(0, far, sib.at[pl.ds(1, n_chips - 1)], True)
        for d in range(1, n_chips):
            for i in range(tp):
                to_sibling(d, i).start()
        gather(far, far, own.at[pl.ds(1, n_chips - 1)], False)
        for i in range(tb):
            for jj in range(g):
                it = ((x + jj) % g) * tb + i
                for d in range(1, n_chips):
                    to_sibling(d, it).wait_recv()
                    own[d, it] = own[d, it] + from_sib[d, it]
                    to_chip(d, it).start()
    gather(2 * far, tp, sib.at[pl.ds(0, 1)], n_chips == 1)
    for i in range(tp):
        to_sibling(0, i).start()
    gather(2 * far + tp, tp, own.at[pl.ds(0, 1)], False)

    w1_copy.wait()
    w2_copy.wait()
    for n in range(min(LEAD, units)):
        relay(n)

    def decode(n, carry):
        @pl.when(n + LEAD < units)
        def _():
            relay(n + LEAD)

        i, j, qq = unit_of(n)
        tile = j * tb + i

        @pl.when((n // g) % n_chips == 0)
        def _():
            to_sibling(0, tile).wait_recv()
            total = own[0, tile] + from_sib[0, tile]
            for d in range(1, n_chips):
                to_chip(d, tile).wait_recv()
                total = total + from_chip[d - 1, tile]
            block[tile] = total

        start = pl.multiple_of(qq * rows_u, rows_u)
        interp = jnp.dot(
            weights[tile, pl.ds(start, rows_u), :], block[tile], preferred_element_type=jnp.float32
        ).astype(jnp.bfloat16)
        v = jnp.dot(interp, w1[...], preferred_element_type=jnp.float32) + w_b1[...]
        half = 0.5 * v
        hidden = (half * jnp.tanh(half) + half).astype(jnp.bfloat16)
        second = jnp.dot(hidden, w2[...], preferred_element_type=jnp.float32) + w_b2[...]
        centred = second - jnp.mean(second, axis=-1, keepdims=True)
        variance = jnp.mean(centred * centred, axis=-1, keepdims=True)
        normed = (centred * lax.rsqrt(variance + 1e-05) * w_gain[...]).astype(jnp.bfloat16)
        result = lax.dot_general(
            w_out[...], normed, (((1,), (1,)), ((), ())), preferred_element_type=jnp.float32
        )
        at = pl.multiple_of(tile * (np_ * cl) + start, rows_u)
        out[:, pl.ds(at, rows_u)] = result + w_bo[...]
        return carry

    lax.fori_loop(0, units, decode, 0)

    @pl.when(p != home)
    def _():
        for src, dst, recv, send in piece_copies:
            remote(src, dst, send, recv, b, home).wait_send()

    for d in range(n_chips):
        for i in range(tp):
            to_sibling(d, i).wait_send()
            if d:
                to_chip(d, i).wait_send()

    def drain(n, carry):
        forwards(n, lambda copy: copy.wait_send())
        return carry

    lax.fori_loop(0, units, drain, 0)


def solution(mesh):
    nb, np_ = mesh.shape["band"], mesh.shape["patch"]

    def body(
        latents, owners, block_rows, pieces, w_first, b_first, w_second, b_second, gain, w_out, b_out
    ):
        tiles, blk = block_rows.shape
        cl, channels = pieces.shape[1], w_out.shape[1]
        mesh_dev, width = latents.shape[1:]
        n_chips, tb, tp = np_ // 2, tiles // nb, tiles // np_
        g = tp // tb
        units = g * tb * n_chips
        depth = next(k for k in (512, 256, 128, mesh_dev) if mesh_dev % k == 0)
        group = max(n_chips - 1, 1) * tp * blk
        vmem = pl.BlockSpec(memory_space=pltpu.VMEM)
        hbm = pl.BlockSpec(memory_space=pl.ANY)
        bf16 = jnp.bfloat16
        dma = pltpu.SemaphoreType.DMA
        result = pl.pallas_call(
            functools.partial(kernel, nb, np_, tiles, blk, cl),
            out_shape=jax.ShapeDtypeStruct((channels, tp * np_ * cl), jnp.float32),
            in_specs=[pl.BlockSpec(memory_space=pltpu.SMEM)] + [vmem] * 6 + [hbm] * 4,
            out_specs=vmem,
            scratch_shapes=[
                pltpu.VMEM((mesh_dev, width), bf16),
                pltpu.VMEM(w_first.shape[1:], bf16),
                pltpu.VMEM(w_second.shape[1:], bf16),
                pltpu.VMEM((blk, blk), jnp.int32),
                pltpu.VMEM((group, depth), bf16),
                pltpu.VMEM((group, width), jnp.float32),
                pltpu.VMEM((n_chips, tp, blk, width), bf16),
                pltpu.VMEM((n_chips, tp, blk, width), bf16),
                pltpu.VMEM((n_chips, tp, blk, width), bf16),
                pltpu.VMEM((max(n_chips - 1, 1), tp, blk, width), bf16),
                pltpu.VMEM((tp, np_ * cl, blk), bf16),
                pltpu.VMEM((tp, blk, width), bf16),
                dma((mesh_dev // depth,)),
                dma((2,)),
                dma((tb,)),
                dma((g, tb, n_chips)),
                dma((3, units)),
                dma((n_chips, tp)),
                dma((n_chips, tp)),
                dma((max(n_chips - 1, 1), tp)),
                dma((max(n_chips - 1, 1), tp)),
            ],
            compiler_params=pltpu.CompilerParams(collective_id=0, has_side_effects=True),
            name="decode",
        )(
            owners, block_rows, b_first, b_second, gain, w_out[0], b_out.reshape(channels, 1),
            latents[0], pieces, w_first[0], w_second[0],
        )
        return result[None]

    return jax.shard_map(
        body,
        mesh=mesh,
        in_specs=(
            P("band", "patch", None),
            P(),
            P(),
            P("band", "patch", None),
            P("band", None, None),
            P("band", None),
            P("band", None, None),
            P("band", None),
            P("band", None),
            P("band", None, None),
            P("band", None),
        ),
        out_specs=P("band", None, "patch"),
        check_vma=False,
    )
```

```python
import functools

import jax
import jax.numpy as jnp
from jax import lax
from jax.experimental import pallas as pl
from jax.experimental.pallas import tpu as pltpu
from jax.sharding import PartitionSpec as P

LEAD = 2


def kernel(
    nb, np_, tiles, blk, cl,
    owners, rows, w_b1, w_b2, w_gain, w_out, w_bo, latents, pieces, w_first, w_second,
    out,
    lat, w1, w2, perm, onehot, acc, sib, own, from_sib, from_chip, weights, block,
    lat_sem, wt_sem, piece_send, w_recv, w_send, sib_send, sib_recv, chip_send, chip_recv,
):
    b, p = lax.axis_index("band"), lax.axis_index("patch")
    n_chips = np_ // 2
    tb, tp = tiles // nb, tiles // np_
    g = tp // tb
    n_z = nb // 2
    q, c = p // 2, p % 2
    z, x = b // 2, b % 2
    units = g * tb * n_chips
    rows_u = 2 * cl
    mesh_dev, width = latents.shape
    depth = onehot.shape[1]
    mesh_type = pl.DeviceIdType.MESH

    def dev(band, patch):
        return {"band": band, "patch": patch}

    def remote(src, dst, send, recv, band, patch):
        return pltpu.make_async_remote_copy(
            src_ref=src, dst_ref=dst, send_sem=send, recv_sem=recv,
            device_id=dev(band, patch), device_id_type=mesh_type,
        )

    barrier = pltpu.get_barrier_semaphore()

    def greet(band, patch):
        pl.semaphore_signal(barrier, inc=1, device_id=dev(band, patch), device_id_type=mesh_type)

    for d in range(1, np_):
        greet(b, (p + d) % np_)
    greet(2 * z + 1 - x, p)

    @pl.when(z > 0)
    def _():
        greet(b - 2, p)

    @pl.when(z < n_z - 1)
    def _():
        greet(b + 2, p)

    lat_copies = [
        pltpu.make_async_copy(
            latents.at[pl.ds(k * depth, depth)], lat.at[pl.ds(k * depth, depth)], lat_sem.at[k]
        )
        for k in range(mesh_dev // depth)
    ]
    for copy in lat_copies:
        copy.start()
    w1_copy = pltpu.make_async_copy(w_first, w1, wt_sem.at[0])
    w2_copy = pltpu.make_async_copy(w_second, w2, wt_sem.at[1])
    w1_copy.start()
    w2_copy.start()

    offsets = list(range(1, n_chips)) + [0]
    order = []
    for d_list in (offsets[:-1], offsets[-1:]):
        for core in (1 - c, c):
            for d in d_list:
                for i in range(tp):
                    order.append((2 * ((q + d) % n_chips) + core) * tp + i)
    perm[...] = jnp.full(perm.shape, -1, jnp.int32)
    for k, t in enumerate(order):
        mine = (owners[t] == p).astype(jnp.int32)
        perm[k : k + 1, :] = rows[pl.ds(t, 1), :] * mine + (mine - 1)
    columns = perm[...].T

    pl.semaphore_wait(barrier, np_ + (z > 0).astype(jnp.int32) + (z < n_z - 1).astype(jnp.int32))

    home = b // g
    own_source = b % g
    piece_copies = [
        (
            pieces.at[i],
            weights.at[own_source * tb + i, pl.ds(pl.multiple_of(p * cl, cl), cl)],
            w_recv.at[own_source, i, p],
            piece_send.at[i],
        )
        for i in range(tb)
    ]

    @pl.when(p == home)
    def _():
        for src, dst, recv, _ in piece_copies:
            pltpu.make_async_copy(src, dst, recv).start()

    @pl.when(p != home)
    def _():
        for src, dst, recv, send in piece_copies:
            remote(src, dst, send, recv, b, home).start()

    def unit_of(n):
        jj, k = n % g, n // g
        i, dd = k // n_chips, k % n_chips
        j = (x + jj) % g
        qq = (q + dd) % n_chips
        return i, j, qq

    def piece(n, half):
        i, j, qq = unit_of(n)
        at = qq * 2 + half
        part = weights.at[j * tb + i, pl.ds(pl.multiple_of(at * cl, cl), cl)]
        return part, w_recv.at[j, i, at]

    def line_of(n):
        source = p * g + unit_of(n)[1]
        return source // 2, x == source % 2

    def forwards(n, half, act):
        zs, on_line = line_of(n)
        part, recv = piece(n, half)
        slot = 2 * n + half

        @pl.when(on_line & (z >= zs) & (z < n_z - 1))
        def _():
            act(remote(part, part, w_send.at[0, slot], recv, b + 2, p))

        @pl.when(on_line & (z <= zs) & (z > 0))
        def _():
            act(remote(part, part, w_send.at[1, slot], recv, b - 2, p))

        @pl.when(on_line)
        def _():
            act(remote(part, part, w_send.at[2, slot], recv, 2 * z + 1 - x, p))

    def arrive(n, half):
        part, recv = piece(n, half)
        pltpu.make_async_copy(part, part, recv).wait()

    def relay(n, at_source):
        zs, on_line = line_of(n)

        @pl.when(on_line & ((z == zs) if at_source else (z != zs)))
        def _():
            for half in range(2):
                arrive(n, half)
                forwards(n, half, lambda copy: copy.start())

    def relay_range(first, last):
        lax.fori_loop(first, last, lambda n, carry: (relay(n, True), carry)[1], 0)

    iota = lax.broadcasted_iota(jnp.int32, (blk, depth), 1)

    def gather(first, count, dst, first_time):
        for k in range(mesh_dev // depth):
            if first_time:
                lat_copies[k].wait()
            for r in range(count):
                hit = iota == (columns[:, first + r : first + r + 1] - k * depth)
                onehot[r * blk : (r + 1) * blk, :] = jnp.where(hit, 1.0, 0.0).astype(jnp.bfloat16)
            part = jnp.dot(
                onehot[: count * blk, :], lat[k * depth : (k + 1) * depth, :],
                preferred_element_type=jnp.float32,
            )
            if k:
                part = part + acc[: count * blk, :]
            if k < mesh_dev // depth - 1:
                acc[: count * blk, :] = part
            else:
                dst[...] = part.astype(jnp.bfloat16).reshape(dst.shape)

    def to_sibling(d, i):
        return remote(
            sib.at[d, i], from_sib.at[d, i], sib_send.at[d, i], sib_recv.at[d, i], b, 2 * q + 1 - c
        )

    def to_chip(d, i):
        return remote(
            own.at[d, i], from_chip.at[d - 1, i], chip_send.at[d - 1, i], chip_recv.at[d - 1, i],
            b, 2 * ((q + d) % n_chips) + c,
        )

    far = (n_chips - 1) * tp
    cut = [units // 4, units // 2, units] if n_chips > 1 else [0, 0, units]
    if n_chips > 1:
        gather(0, far, sib.at[pl.ds(1, n_chips - 1)], True)
        for d in range(1, n_chips):
            for i in range(tp):
                to_sibling(d, i).start()
        relay_range(0, cut[0])
        gather(far, far, own.at[pl.ds(1, n_chips - 1)], False)
        for i in range(tb):
            for jj in range(g):
                it = ((x + jj) % g) * tb + i
                for d in range(1, n_chips):
                    to_sibling(d, it).wait_recv()
                    own[d, it] = own[d, it] + from_sib[d, it]
                    to_chip(d, it).start()
    relay_range(cut[0], cut[1])
    gather(2 * far, tp, sib.at[pl.ds(0, 1)], n_chips == 1)
    for i in range(tp):
        to_sibling(0, i).start()
    relay_range(cut[1], cut[2])
    gather(2 * far + tp, tp, own.at[pl.ds(0, 1)], False)

    w1_copy.wait()
    w2_copy.wait()
    for n in range(min(LEAD, units)):
        relay(n, False)

    channels = w_bo.shape[1]
    eye = lax.broadcasted_iota(jnp.int32, (channels, channels), 0) == lax.broadcasted_iota(
        jnp.int32, (channels, channels), 1
    )
    bias = jnp.sum(jnp.where(eye, w_bo[...], 0.0), axis=1, keepdims=True)

    def decode(n, carry):
        @pl.when(n + LEAD < units)
        def _():
            relay(n + LEAD, False)

        @pl.when(jnp.logical_not(line_of(n)[1]))
        def _():
            for half in range(2):
                arrive(n, half)

        i, j, qq = unit_of(n)
        tile = j * tb + i

        @pl.when((n // g) % n_chips == 0)
        def _():
            to_sibling(0, tile).wait_recv()
            total = own[0, tile] + from_sib[0, tile]
            for d in range(1, n_chips):
                to_chip(d, tile).wait_recv()
                total = total + from_chip[d - 1, tile]
            block[tile] = total

        start = pl.multiple_of(qq * rows_u, rows_u)
        interp = jnp.dot(
            weights[tile, pl.ds(start, rows_u), :], block[tile], preferred_element_type=jnp.float32
        ).astype(jnp.bfloat16)
        v = jnp.dot(interp, w1[...], preferred_element_type=jnp.float32) + w_b1[...]
        half = 0.5 * v
        hidden = (half * jnp.tanh(half) + half).astype(jnp.bfloat16)
        second = jnp.dot(hidden, w2[...], preferred_element_type=jnp.float32) + w_b2[...]
        centred = second - jnp.mean(second, axis=-1, keepdims=True)
        variance = jnp.mean(centred * centred, axis=-1, keepdims=True)
        normed = (centred * lax.rsqrt(variance + 1e-05) * w_gain[...]).astype(jnp.bfloat16)
        result = lax.dot_general(
            w_out[...], normed, (((1,), (1,)), ((), ())), preferred_element_type=jnp.float32
        )
        at = pl.multiple_of(tile * (np_ * cl) + start, rows_u)
        result = result + bias
        for ch in range(channels):
            out[ch, :, pl.ds(at, rows_u)] = result[ch : ch + 1]
        return carry

    lax.fori_loop(0, units, decode, 0)

    @pl.when(p != home)
    def _():
        for src, dst, recv, send in piece_copies:
            remote(src, dst, send, recv, b, home).wait_send()

    for d in range(n_chips):
        for i in range(tp):
            to_sibling(d, i).wait_send()
            if d:
                to_chip(d, i).wait_send()

    def drain(n, carry):
        for half in range(2):
            forwards(n, half, lambda copy: copy.wait_send())
        return carry

    lax.fori_loop(0, units, drain, 0)


def solution(mesh):
    nb, np_ = mesh.shape["band"], mesh.shape["patch"]

    def body(
        latents, owners, block_rows, pieces, w_first, b_first, w_second, b_second, gain, w_out, b_out
    ):
        tiles, blk = block_rows.shape
        cl, channels = pieces.shape[1], w_out.shape[1]
        mesh_dev, width = latents.shape[1:]
        n_chips, tb, tp = np_ // 2, tiles // nb, tiles // np_
        g = tp // tb
        units = g * tb * n_chips
        depth = next(k for k in (512, 256, 128, mesh_dev) if mesh_dev % k == 0)
        group = max(n_chips - 1, 1) * tp * blk
        vmem = pl.BlockSpec(memory_space=pltpu.VMEM)
        hbm = pl.BlockSpec(memory_space=pl.ANY)
        bf16 = jnp.bfloat16
        dma = pltpu.SemaphoreType.DMA
        result = pl.pallas_call(
            functools.partial(kernel, nb, np_, tiles, blk, cl),
            out_shape=jax.ShapeDtypeStruct((channels, 1, tp * np_ * cl), jnp.float32),
            in_specs=[pl.BlockSpec(memory_space=pltpu.SMEM)] + [vmem] * 6 + [hbm] * 4,
            out_specs=vmem,
            scratch_shapes=[
                pltpu.VMEM((mesh_dev, width), bf16),
                pltpu.VMEM(w_first.shape[1:], bf16),
                pltpu.VMEM(w_second.shape[1:], bf16),
                pltpu.VMEM((blk, blk), jnp.int32),
                pltpu.VMEM((group, depth), bf16),
                pltpu.VMEM((group, width), jnp.float32),
                pltpu.VMEM((n_chips, tp, blk, width), bf16),
                pltpu.VMEM((n_chips, tp, blk, width), bf16),
                pltpu.VMEM((n_chips, tp, blk, width), bf16),
                pltpu.VMEM((max(n_chips - 1, 1), tp, blk, width), bf16),
                pltpu.VMEM((tp, np_ * cl, blk), bf16),
                pltpu.VMEM((tp, blk, width), bf16),
                dma((mesh_dev // depth,)),
                dma((2,)),
                dma((tb,)),
                dma((g, tb, np_)),
                dma((3, 2 * units)),
                dma((n_chips, tp)),
                dma((n_chips, tp)),
                dma((max(n_chips - 1, 1), tp)),
                dma((max(n_chips - 1, 1), tp)),
            ],
            compiler_params=pltpu.CompilerParams(collective_id=0, has_side_effects=True),
            name="decode",
        )(
            owners, block_rows, b_first, b_second, gain, w_out[0], b_out,
            latents[0], pieces, w_first[0], w_second[0],
        )
        return jnp.transpose(result, (1, 0, 2))

    return jax.shard_map(
        body,
        mesh=mesh,
        in_specs=(
            P("band", "patch", None),
            P(),
            P(),
            P("band", "patch", None),
            P("band", None, None),
            P("band", None),
            P("band", None, None),
            P("band", None),
            P("band", None),
            P("band", None, None),
            P("band", None),
        ),
        out_specs=P("band", None, "patch"),
        check_vma=False,
    )
```
